32 devices in a mesh: kpt: 2 (over x), gx: 16 (over z, y, core).
Axes of the slice: x: 2, y: 2, z: 4, core: 2. Of those that a mesh axis runs over, the one named last changes fastest.
Arguments:
- e_field: float32 [2, 3, 64, 512, 128], P(None, None, ('kpt', 'gx')), parts along dimension 2, may hold values from -6 to 6
- h_field: float32 [2, 3, 64, 512, 128], P(None, None, ('kpt', 'gx')), parts along dimension 2, may hold values from -6 to 6
- labels: int32 [64, 512, 128], P(('kpt', 'gx')), parts along dimension 0, may hold values from 0 to 3
- kpoint: int32 [4], P('kpt'), parts along dimension 0, may hold values from 0 to 15
- eps_inf: float32 [4], replicated, may hold values from 1 to 12
- delta_eps: float32 [4], replicated, may hold values from 0.5 to 4
- omega_zero: float32 [4], replicated, may hold values from 0.2 to 1
- damping: float32 [4], replicated, may hold values from 0.05 to 0.8
Outputs:
- e_final: float32 [2, 3, 64, 512, 128], P(None, None, ('kpt', 'gx')), parts along dimension 2
- h_final: float32 [2, 3, 64, 512, 128], P(None, None, ('kpt', 'gx')), parts along dimension 2
The draws below stay inside these ranges and needn't reach their ends.
There are 2 independent parts, one for each index of `kpt`. The reference program is written for one: setup_inputs(seed, part) draws one part's arguments, and reference() takes and returns one part's arrays. A program takes and returns all parts, laid end to end along the dimension named above; an argument that names none is the same for every part. Nothing has to cross between parts.
Inputs may be any that keep to these rules, and one draw needn't show every extreme that they name: `kpoint`: entry 0 indexes the k-point along x, entry 1 along y, out of 16 each.
All inputs are finite; a program needn't handle non-finite values.
Results may differ from the reference program's by a relative error of at most 0.00002.
Values sent between devices are 32-bit elements; how exact they have to be, the bound alone decides.
A program may use at most 128 MiB of HBM per device.

```python
import math
import jax
import jax.numpy as jnp
from jax import lax

NY = 512
NZ = 128
ITERS = 12
LABELS = 4
KGRID = 16
NX = 32


def with_ends(entries, key, least, top_value):
    spot = [jax.random.randint(jax.random.fold_in(key, axis), (), 0, length) for axis, length in enumerate(entries.shape)]
    longest = entries.shape.index(max(entries.shape))
    beside = spot[:longest] + [(spot[longest] + 1) % entries.shape[longest]] + spot[longest + 1:]
    return entries.at[tuple(spot)].set(least).at[tuple(beside)].set(top_value)


def level_of(key, shape, split, smallest, largest):
    def one(dim, parts):
        draws = jax.random.uniform(jax.random.fold_in(jax.random.fold_in(key, 6), dim), (parts,), jnp.float32, smallest / len(split), largest / len(split))
        return jnp.repeat(jnp.exp(draws), shape[dim] // parts).reshape((-1,) + (1,) * (len(shape) - dim - 1))

    factor_of = one(*split[0])
    for cut in split[1:]:
        factor_of = factor_of * one(*cut)
    return factor_of


def noise(stream_key, shape, scale, bound, split=(), held_as=jnp.bfloat16):
    array = jax.random.normal(stream_key, shape, jnp.float32) * scale
    if len(split) > 0:
        array = level_of(stream_key, shape, split, -0.22, 0.18) * array
    return jnp.clip(array, min=-bound, max=bound).astype(held_as)


def setup_inputs(seed: int = 0, part: int = 0) -> dict:
    key_of = jax.random.split(jax.random.key(seed), 9)
    part_splits = jax.random.split(jax.random.fold_in(key_of[8], part), 9)
    return {
        "e_field": noise(part_splits[0], (2, 3, NX, NY, NZ), 1.0, 6.0, ((2, 16),), jnp.float32),
        "h_field": noise(part_splits[1], (2, 3, NX, NY, NZ), 1.0, 6.0, ((2, 16),), jnp.float32),
        "labels": with_ends(jax.random.randint(part_splits[2], (NX, NY, NZ), 0, LABELS), jax.random.fold_in(part_splits[2], 1), 0, LABELS - 1).astype(jnp.int32),
        "kpoint": jax.random.randint(part_splits[3], (2,), 0, KGRID).astype(jnp.int32),
        "eps_inf": jnp.clip(jnp.exp(jax.random.uniform(key_of[4], (LABELS,), jnp.float32, math.log(1.0), math.log(12.0))), 1.0, 12.0),
        "delta_eps": jnp.clip(jnp.exp(jax.random.uniform(key_of[5], (LABELS,), jnp.float32, math.log(0.5), math.log(4.0))), 0.5, 4.0),
        "omega_zero": jnp.clip(jnp.exp(jax.random.uniform(key_of[6], (LABELS,), jnp.float32, math.log(0.2), math.log(1.0))), 0.2, 1.0),
        "damping": jnp.clip(jnp.exp(jax.random.uniform(key_of[7], (LABELS,), jnp.float32, math.log(0.05), math.log(0.8))), 0.05, 0.8),
    }


time_step = 0.5


def cmul(field, cosv, sinv):
    return jnp.stack([field[0] * cosv - field[1] * sinv, field[0] * sinv + field[1] * cosv])


def next_axis(field, axis, cosv, sinv):
    rolled = jnp.roll(field, -1, axis=axis)
    count = field.shape[axis]
    inner = lax.slice_in_dim(rolled, 0, count - 1, axis=axis)
    last = cmul(lax.slice_in_dim(rolled, count - 1, count, axis=axis), cosv, sinv)
    return jnp.concatenate([inner, last], axis=axis)


def prev_axis(field, axis, cosv, sinv):
    rolled = jnp.roll(field, 1, axis=axis)
    count = field.shape[axis]
    first = cmul(lax.slice_in_dim(rolled, 0, 1, axis=axis), cosv, -sinv)
    inner = lax.slice_in_dim(rolled, 1, count, axis=axis)
    return jnp.concatenate([first, inner], axis=axis)


def next_z(field):
    zeros = jnp.zeros(field.shape[:-1] + (1,), jnp.float32)
    return jnp.concatenate([field[..., 1:], zeros], axis=-1)


def prev_z(field):
    zeros = jnp.zeros(field.shape[:-1] + (1,), jnp.float32)
    return jnp.concatenate([zeros, field[..., :-1]], axis=-1)


def per_cell(labels, table):
    picked = jnp.zeros(labels.shape, jnp.float32)
    for label in range(table.shape[0]):
        picked = picked + jnp.where(labels == label, table[label], jnp.float32(0.0))
    return picked


def reference(e_field, h_field, labels, kpoint, eps_inf, delta_eps, omega_zero, damping):
    theta_x = jnp.float32(2.0 * math.pi) * kpoint[0].astype(jnp.float32) / KGRID
    theta_y = jnp.float32(2.0 * math.pi) * kpoint[1].astype(jnp.float32) / KGRID
    cos_x, sin_x = jnp.cos(theta_x), jnp.sin(theta_x)
    cos_y, sin_y = jnp.cos(theta_y), jnp.sin(theta_y)
    half = damping * time_step / 2.0
    ce = per_cell(labels, time_step / eps_inf)
    ja = per_cell(labels, (1.0 - half) / (1.0 + half))
    jb = per_cell(labels, time_step * omega_zero * omega_zero / (1.0 + half))
    de = per_cell(labels, delta_eps)

    def advance(step, carry):
        efield, hfield, polar, current = carry
        ex, ey, ez = efield[:, 0], efield[:, 1], efield[:, 2]
        curl_x = (next_axis(ez, -2, cos_y, sin_y) - ez) - (next_z(ey) - ey)
        curl_y = (next_z(ex) - ex) - (next_axis(ez, -3, cos_x, sin_x) - ez)
        curl_z = (next_axis(ey, -3, cos_x, sin_x) - ey) - (next_axis(ex, -2, cos_y, sin_y) - ex)
        hfield = hfield - time_step * jnp.stack([curl_x, curl_y, curl_z], axis=1)
        hx, hy, hz = hfield[:, 0], hfield[:, 1], hfield[:, 2]
        kurl_x = (hz - prev_axis(hz, -2, cos_y, sin_y)) - (hy - prev_z(hy))
        kurl_y = (hx - prev_z(hx)) - (hz - prev_axis(hz, -3, cos_x, sin_x))
        kurl_z = (hy - prev_axis(hy, -3, cos_x, sin_x)) - (hx - prev_axis(hx, -2, cos_y, sin_y))
        kurl = jnp.stack([kurl_x, kurl_y, kurl_z], axis=1)
        current = ja * current + jb * (de * efield - polar)
        polar = polar + time_step * current
        efield = efield + ce * (kurl - current)
        return efield, hfield, polar, current

    zeros = jnp.zeros(e_field.shape, jnp.float32)
    efield, hfield, polar, current = lax.fori_loop(0, ITERS, advance, (e_field, h_field, zeros, zeros))
    return efield, hfield
```

```python
import functools
import math

import jax
import jax.numpy as jnp
from jax import lax
from jax.experimental import pallas as pl
from jax.experimental.pallas import tpu as pltpu
from jax.sharding import PartitionSpec as P

ITERS = 12
KGRID = 16
CHUNKS = 8
BLOCK = 8
UNROLL = 2
PAD = 8

time_step = 0.5


def kernel(e_in, h_in, lab_in, table, phase, e_out, h_out,
           e, h, pol, cur, coef, lab, ge, gh,
           in_sem, out_sem, se_sem, re_sem, sh_sem, rh_sem):
    planes, rows, width = lab.shape
    chunk = rows // CHUNKS
    gx = lax.axis_size("gx")
    me = lax.axis_index("gx")
    right, left = lax.rem(me + 1, gx), lax.rem(me + gx - 1, gx)
    last = planes - 1

    def rows_of(c):
        return pl.ds(pl.multiple_of(c * chunk, chunk), chunk)

    def h_rows_of(c):
        return pl.ds(pl.multiple_of(c * chunk + PAD, 8), chunk)

    loads = [
        pltpu.make_async_copy(e_in, e.at[:, :, :, pl.ds(0, rows)], in_sem.at[0]),
        pltpu.make_async_copy(lab_in, lab, in_sem.at[2]),
        pltpu.make_async_copy(h_in, h.at[:, :, :, pl.ds(PAD, rows)], in_sem.at[1]),
    ]
    for load in loads:
        load.start()

    barrier = pltpu.get_barrier_semaphore()
    for other in (left, right):
        pl.semaphore_signal(barrier, inc=1, device_id={"gx": other},
                            device_id_type=pl.DeviceIdType.MESH)
    pl.semaphore_wait(barrier, 2)

    def send_e(c, source):
        return pltpu.make_async_remote_copy(
            src_ref=source.at[:, pl.ds(1, 2), 0, rows_of(c)],
            dst_ref=ge.at[:, :, rows_of(c)],
            send_sem=se_sem.at[c], recv_sem=re_sem.at[c],
            device_id={"gx": left}, device_id_type=pl.DeviceIdType.MESH)

    def send_h(c):
        return pltpu.make_async_remote_copy(
            src_ref=h.at[:, pl.ds(1, 2), last, h_rows_of(c)],
            dst_ref=gh.at[:, :, rows_of(c)],
            send_sem=sh_sem.at[c], recv_sem=rh_sem.at[c],
            device_id={"gx": right}, device_id_type=pl.DeviceIdType.MESH)

    def store_out(c):
        return pltpu.make_async_copy(e.at[:, :, :, rows_of(c)],
                                     e_out.at[:, :, :, rows_of(c)], out_sem.at[c])

    def store_h_out(c):
        return pltpu.make_async_copy(h.at[:, :, :, h_rows_of(c)],
                                     h_out.at[:, :, :, rows_of(c)], out_sem.at[CHUNKS + c])

    @pl.loop(0, CHUNKS)
    def _(c):
        send_e(c, e_in).start()

    zero = jnp.zeros((BLOCK, width), jnp.float32)

    loads[1].wait()

    @pl.loop(0, rows // BLOCK)
    def _(i):
        here = pl.ds(pl.multiple_of(i * BLOCK, BLOCK), BLOCK)
        for x in range(planes):
            label = lab[x, here]
            masks = [label == k for k in range(table.shape[1])]
            for which in range(4):
                picked = zero
                for k, mask in enumerate(masks):
                    picked = picked + jnp.where(mask, table[which, k], jnp.float32(0.0))
                coef[which, x, here] = picked
            for ri in range(2):
                for a in range(3):
                    pol[ri, a, x, here] = zero
                    cur[ri, a, x, here] = zero

    cos_r, sin_r, cos_l, sin_l, cos_y, sin_y = [phase[i] for i in range(6)]
    lane = lax.broadcasted_iota(jnp.int32, (BLOCK, width), 1)
    not_end = lane < width - 1
    not_start = lane > 0

    def wrap_e():
        for a in (0, 2):
            for x in range(planes):
                re, im = e[0, a, x, 0:1], e[1, a, x, 0:1]
                e[0, a, x, rows:rows + 1] = re * cos_y - im * sin_y
                e[1, a, x, rows:rows + 1] = re * sin_y + im * cos_y

    def wrap_h():
        end = PAD + rows - 1
        for a in (0, 2):
            for x in range(planes):
                re, im = h[0, a, x, end:end + 1], h[1, a, x, end:end + 1]
                h[0, a, x, PAD - 1:PAD] = re * cos_y + im * sin_y
                h[1, a, x, PAD - 1:PAD] = im * cos_y - re * sin_y

    def turned(re, im, cosv, sinv):
        return re * cosv - im * sinv, re * sinv + im * cosv

    def next_z(f):
        return jnp.where(not_end, pltpu.roll(f, width - 1, 1), 0.0)

    def prev_z(f):
        return jnp.where(not_start, pltpu.roll(f, 1, 1), 0.0)

    def magnetic(x, r):
        here = pl.ds(pl.multiple_of(r, BLOCK), BLOCK)
        there = pl.ds(pl.multiple_of(r + PAD, 8), BLOCK)
        up = pl.ds(r + 1, BLOCK)
        if x == last:
            beyond = [turned(ge[0, a, here], ge[1, a, here], cos_r, sin_r) for a in range(2)]
        else:
            beyond = [(e[0, a, x + 1, here], e[1, a, x + 1, here]) for a in (1, 2)]
        for ri in range(2):
            ex, ey, ez = [e[ri, a, x, here] for a in range(3)]
            cx = (e[ri, 2, x, up] - ez) - (next_z(ey) - ey)
            cy = (next_z(ex) - ex) - (beyond[1][ri] - ez)
            cz = (beyond[0][ri] - ey) - (e[ri, 0, x, up] - ex)
            for a, curl in enumerate((cx, cy, cz)):
                h[ri, a, x, there] = h[ri, a, x, there] - time_step * curl

    def electric(x, r):
        here = pl.ds(pl.multiple_of(r, BLOCK), BLOCK)
        there = pl.ds(pl.multiple_of(r + PAD, 8), BLOCK)
        down = pl.ds(r + PAD - 1, BLOCK)
        ce, ja, jb, de = [coef[k, x, here] for k in range(4)]
        if x == 0:
            before = [turned(gh[0, a, here], gh[1, a, here], cos_l, sin_l) for a in range(2)]
        else:
            before = [(h[0, a, x - 1, there], h[1, a, x - 1, there]) for a in (1, 2)]
        for ri in range(2):
            hx, hy, hz = [h[ri, a, x, there] for a in range(3)]
            kx = (hz - h[ri, 2, x, down]) - (hy - prev_z(hy))
            ky = (hx - prev_z(hx)) - (hz - before[1][ri])
            kz = (hy - before[0][ri]) - (hx - h[ri, 0, x, down])
            for a, kurl in enumerate((kx, ky, kz)):
                field, polar = e[ri, a, x, here], pol[ri, a, x, here]
                current = ja * cur[ri, a, x, here] + jb * (de * field - polar)
                cur[ri, a, x, here] = current
                pol[ri, a, x, here] = polar + time_step * current
                e[ri, a, x, here] = field + ce * (kurl - current)

    def sweep(update, order, c):
        def one(i, carry):
            for x in order:
                update(x, c * chunk + i * BLOCK)
            return carry
        lax.fori_loop(0, chunk // BLOCK, one, 0, unroll=UNROLL)

    loads[0].wait()
    loads[2].wait()
    wrap_e()

    @pl.loop(0, ITERS)
    def _(step):
        @pl.loop(0, CHUNKS)
        def _(c):
            @pl.when(step > 0)
            def _():
                send_h(c).wait_send()
            send_e(c, e).wait_recv()
            sweep(magnetic, range(planes - 1, -1, -1), c)
            send_h(c).start()

        wrap_h()

        @pl.when(step == ITERS - 1)
        def _():
            @pl.loop(0, CHUNKS)
            def _(c):
                store_h_out(c).start()

        @pl.loop(0, CHUNKS)
        def _(c):
            send_e(c, e).wait_send()
            send_h(c).wait_recv()
            sweep(electric, range(planes), c)

            @pl.when(step < ITERS - 1)
            def _():
                send_e(c, e).start()

            @pl.when(step == ITERS - 1)
            def _():
                store_out(c).start()

        wrap_e()

    @pl.loop(0, CHUNKS)
    def _(c):
        send_h(c).wait_send()
        store_h_out(c).wait()
        store_out(c).wait()


def shards(e_field, h_field, labels, kpoint, eps_inf, delta_eps, omega_zero, damping):
    theta_x = jnp.float32(2.0 * math.pi) * kpoint[0].astype(jnp.float32) / KGRID
    theta_y = jnp.float32(2.0 * math.pi) * kpoint[1].astype(jnp.float32) / KGRID
    cos_x, sin_x = (jnp.cos(theta_x), jnp.sin(theta_x))
    cos_y, sin_y = (jnp.cos(theta_y), jnp.sin(theta_y))
    half = damping * time_step / 2.0
    table = jnp.stack([
        time_step / eps_inf,
        (1.0 - half) / (1.0 + half),
        time_step * omega_zero * omega_zero / (1.0 + half),
        delta_eps,
    ])
    position = lax.axis_index("gx")
    at_first = position == 0
    at_last = position == lax.axis_size("gx") - 1
    one, nought = jnp.float32(1.0), jnp.float32(0.0)
    phase = jnp.stack([
        jnp.where(at_last, cos_x, one), jnp.where(at_last, sin_x, nought),
        jnp.where(at_first, cos_x, one), jnp.where(at_first, -sin_x, nought),
        cos_y, sin_y,
    ])
    planes, rows, width = labels.shape
    state = (2, 3, planes, rows, width)
    padded = (2, 3, planes, rows + PAD, width)
    anywhere = pl.BlockSpec(memory_space=pl.ANY)
    scalars = pl.BlockSpec(memory_space=pltpu.SMEM)
    return pl.pallas_call(
        kernel,
        out_shape=(jax.ShapeDtypeStruct(state, jnp.float32),) * 2,
        in_specs=[anywhere] * 3 + [scalars] * 2,
        out_specs=(anywhere, anywhere),
        scratch_shapes=[
            pltpu.VMEM(padded, jnp.float32),
            pltpu.VMEM(padded, jnp.float32),
            pltpu.VMEM(state, jnp.float32),
            pltpu.VMEM(state, jnp.float32),
            pltpu.VMEM((4, planes, rows, width), jnp.float32),
            pltpu.VMEM((planes, rows, width), jnp.int32),
            pltpu.VMEM((2, 2, rows, width), jnp.float32),
            pltpu.VMEM((2, 2, rows, width), jnp.float32),
            pltpu.SemaphoreType.DMA((3,)),
            pltpu.SemaphoreType.DMA((2 * CHUNKS,)),
            pltpu.SemaphoreType.DMA((CHUNKS,)),
            pltpu.SemaphoreType.DMA((CHUNKS,)),
            pltpu.SemaphoreType.DMA((CHUNKS,)),
            pltpu.SemaphoreType.DMA((CHUNKS,)),
        ],
        compiler_params=pltpu.CompilerParams(collective_id=0, has_side_effects=True),
    )(e_field, h_field, labels, table, phase)


def solution(mesh):
    placed = (
        P(None, None, ("kpt", "gx"), None, None),
        P(None, None, ("kpt", "gx"), None, None),
        P(("kpt", "gx"), None, None),
        P("kpt"),
        P(),
        P(),
        P(),
        P(),
    )
    return jax.shard_map(
        shards,
        mesh=mesh,
        in_specs=placed,
        out_specs=(
            P(None, None, ("kpt", "gx"), None, None),
            P(None, None, ("kpt", "gx"), None, None),
        ),
        check_vma=False,
    )
```

```python
import functools
import math

import jax
import jax.numpy as jnp
from jax import lax
from jax.experimental import pallas as pl
from jax.experimental.pallas import tpu as pltpu
from jax.sharding import PartitionSpec as P

ITERS = 12
KGRID = 16
CHUNKS = 4
BLOCK = 8
UNROLL = 2
PAD = 8

time_step = 0.5


class Tile:
    def __init__(self, refs, sems, left, right, turns):
        self.e, self.h, self.pol, self.cur, self.coef, self.lab, self.ge, self.gh = refs[:8]
        self.e_stage, self.h_stage, self.e_edge, self.h_edge = refs[8:]
        self.se, self.re, self.sh, self.rh = sems
        self.left, self.right = left, right
        self.turn_r, self.turn_l, self.turn_up, self.turn_down = turns
        self.planes, self.rows, self.width = self.lab.shape
        self.chunk = self.rows // CHUNKS

    def send_e(self, c):
        here = pl.ds(c * self.chunk, self.chunk)
        return pltpu.make_async_remote_copy(
            src_ref=self.e.at[:, pl.ds(1, 2), 0, here], dst_ref=self.ge.at[:, :, here],
            send_sem=self.se.at[c], recv_sem=self.re.at[c],
            device_id={"gx": self.left}, device_id_type=pl.DeviceIdType.MESH)

    def send_h(self, c):
        here, there = pl.ds(c * self.chunk, self.chunk), pl.ds(c * self.chunk + PAD, self.chunk)
        return pltpu.make_async_remote_copy(
            src_ref=self.h.at[:, pl.ds(1, 2), self.planes - 1, there], dst_ref=self.gh.at[:, :, here],
            send_sem=self.sh.at[c], recv_sem=self.rh.at[c],
            device_id={"gx": self.right}, device_id_type=pl.DeviceIdType.MESH)

    def clear(self, table):
        zero = jnp.zeros((BLOCK, self.width), jnp.float32)

        @pl.loop(0, self.rows // BLOCK)
        def _(i):
            here = pl.ds(pl.multiple_of(i * BLOCK, BLOCK), BLOCK)
            for x in range(self.planes):
                label = self.lab[x, here]
                masks = [label == k for k in range(table.shape[1])]
                for which in range(4):
                    picked = zero
                    for k, mask in enumerate(masks):
                        picked = picked + jnp.where(mask, table[which, k], jnp.float32(0.0))
                    self.coef[which, x, here] = picked
                for ri in range(2):
                    for a in range(3):
                        self.pol[ri, a, x, here] = zero
                        self.cur[ri, a, x, here] = zero

    def stage_e(self):
        for x in range(self.planes):
            for ri in range(2):
                for j, a in enumerate((0, 2)):
                    row = 2 * ri + j
                    self.e_stage[x, row:row + 1] = self.e[ri, a, x, 0:1]

    def stage_h(self):
        end = PAD + self.rows - 1
        for x in range(self.planes):
            for ri in range(2):
                for j, a in enumerate((0, 2)):
                    row = 2 * ri + j
                    self.h_stage[x, row:row + 1] = self.h[ri, a, x, end:end + 1]

    def take_edge(self, edge, field, at, turn):
        for x in range(self.planes):
            for j, a in enumerate((0, 2)):
                re, im = turned(edge[x, j:j + 1], edge[x, 2 + j:3 + j], *turn)
                field[0, a, x, at:at + 1] = re
                field[1, a, x, at:at + 1] = im

    def take_e(self):
        self.take_edge(self.e_edge, self.e, self.rows, self.turn_up)

    def take_h(self):
        self.take_edge(self.h_edge, self.h, PAD - 1, self.turn_down)

    def magnetic(self, x, r, next_z, prev_z):
        e, h, ge = self.e, self.h, self.ge
        here = pl.ds(pl.multiple_of(r, BLOCK), BLOCK)
        there = pl.ds(pl.multiple_of(r + PAD, 8), BLOCK)
        up = pl.ds(r + 1, BLOCK)
        if x == self.planes - 1:
            beyond = [turned(ge[0, a, here], ge[1, a, here], *self.turn_r) for a in range(2)]
        else:
            beyond = [(e[0, a, x + 1, here], e[1, a, x + 1, here]) for a in (1, 2)]
        for ri in range(2):
            ex, ey, ez = [e[ri, a, x, here] for a in range(3)]
            cx = (e[ri, 2, x, up] - ez) - (next_z(ey) - ey)
            cy = (next_z(ex) - ex) - (beyond[1][ri] - ez)
            cz = (beyond[0][ri] - ey) - (e[ri, 0, x, up] - ex)
            for a, curl in enumerate((cx, cy, cz)):
                h[ri, a, x, there] = h[ri, a, x, there] - time_step * curl

    def electric(self, x, r, next_z, prev_z):
        e, h, gh, pol, cur = self.e, self.h, self.gh, self.pol, self.cur
        here = pl.ds(pl.multiple_of(r, BLOCK), BLOCK)
        there = pl.ds(pl.multiple_of(r + PAD, 8), BLOCK)
        down = pl.ds(r + PAD - 1, BLOCK)
        ce, ja, jb, de = [self.coef[k, x, here] for k in range(4)]
        if x == 0:
            before = [turned(gh[0, a, here], gh[1, a, here], *self.turn_l) for a in range(2)]
        else:
            before = [(h[0, a, x - 1, there], h[1, a, x - 1, there]) for a in (1, 2)]
        for ri in range(2):
            hx, hy, hz = [h[ri, a, x, there] for a in range(3)]
            kx = (hz - h[ri, 2, x, down]) - (hy - prev_z(hy))
            ky = (hx - prev_z(hx)) - (hz - before[1][ri])
            kz = (hy - before[0][ri]) - (hx - h[ri, 0, x, down])
            for a, kurl in enumerate((kx, ky, kz)):
                field, polar = e[ri, a, x, here], pol[ri, a, x, here]
                current = ja * cur[ri, a, x, here] + jb * (de * field - polar)
                cur[ri, a, x, here] = current
                pol[ri, a, x, here] = polar + time_step * current
                e[ri, a, x, here] = field + ce * (kurl - current)

    def sweep(self, update, order, c, shifts):
        def one(i, carry):
            for x in order:
                update(x, c * self.chunk + i * BLOCK, *shifts)
            return carry
        lax.fori_loop(0, self.chunk // BLOCK, one, 0, unroll=UNROLL)


def turned(re, im, cosv, sinv):
    return re * cosv - im * sinv, re * sinv + im * cosv


def kernel(e_in, h_in, lab_in, table, phase, e_out, h_out, *scratch):
    gx = lax.axis_size("gx")
    me = lax.axis_index("gx")
    q = lax.rem(me, 4)
    base = me - q
    y = lax.div(q, 2)
    core = lax.rem(q, 2)
    local = lab_in.shape[0]
    own_refs, moved_refs = scratch[:12], scratch[12:24]
    own_sems, moved_sems = scratch[24:28], scratch[28:32]
    in_sem, out_sem, sl, rl, so, ro, ees, eer, hhs, hhr = scratch[32:]
    ph = [phase[i] for i in range(12)]
    one, nought = jnp.float32(1.0), jnp.float32(0.0)
    cos_y, sin_y = ph[8], ph[9]
    own = Tile(own_refs, own_sems, lax.rem(me + gx - 1, gx), lax.rem(me + 1, gx),
               ((ph[0], ph[1]), (ph[2], ph[3]), (one, nought), (cos_y, -sin_y)))
    moved = Tile(moved_refs, moved_sems,
                 lax.rem(me + gx - 3 + 2 * core, gx), lax.rem(me + 3 - 2 * (1 - core), gx),
                 ((ph[4], ph[5]), (ph[6], ph[7]), (ph[10], ph[11]), (one, nought)))
    tiles = (own, moved)
    keep, part, width = own.rows, moved.rows, own.width

    def remote(src, dst, send, recv, to):
        return pltpu.make_async_remote_copy(
            src_ref=src, dst_ref=dst, send_sem=send, recv_sem=recv,
            device_id={"gx": to}, device_id_type=pl.DeviceIdType.MESH)

    loads = [
        pltpu.make_async_copy(lab_in.at[:, pl.ds(0, keep)], own.lab, in_sem.at[0]),
        pltpu.make_async_copy(e_in.at[:, :, :, pl.ds(0, keep)], own.e.at[:, :, :, pl.ds(0, keep)], in_sem.at[1]),
        pltpu.make_async_copy(h_in.at[:, :, :, pl.ds(0, keep)], own.h.at[:, :, :, pl.ds(PAD, keep)], in_sem.at[2]),
    ]
    for load in loads:
        load.start()

    barrier = pltpu.get_barrier_semaphore()
    others = [base + lax.rem(q + k, 4) for k in (1, 2, 3)]
    others += [lax.rem(me + gx + k, gx) for k in (-3, -1, 1, 3)]
    for other in others:
        pl.semaphore_signal(barrier, inc=1, device_id={"gx": other},
                            device_id_type=pl.DeviceIdType.MESH)
    pl.semaphore_wait(barrier, len(others))

    def move_in(half, slot):
        rows = pl.ds(keep + half * part, part)
        planes = pl.ds(slot * local, local)
        return ((e_in.at[:, :, :, rows], moved.e.at[:, :, planes, pl.ds(0, part)]),
                (lab_in.at[:, rows], moved.lab.at[planes]),
                (h_in.at[:, :, :, rows], moved.h.at[:, :, planes, pl.ds(PAD, part)]))

    def each_move_in(act):
        for half in range(2):
            self_q = 3 * half
            for k, (src, dst) in enumerate(move_in(half, self_q % 2)):
                @pl.when(q == self_q)
                def _():
                    act(None, pltpu.make_async_copy(src, dst, rl.at[k, self_q % 2]))
            for slot in range(2):
                for k, (src, dst) in enumerate(move_in(half, slot)):
                    @pl.when((q != self_q) & (core == slot))
                    def _():
                        act(remote(src, dst, sl.at[k, half], rl.at[k, slot], base + 2 * half + y), None)

    each_move_in(lambda far, near: (far or near).start())

    def wait_in(k):
        for slot in range(2):
            src, dst = move_in(0, slot)[k]
            remote(src, dst, sl.at[k, 0], rl.at[k, slot], base + lax.rem(q + 1, 4)).wait_recv()

    def edges(f, o_stage, a_stage, o_edge, a_edge, ss, rs, act):
        for slot in range(2):
            src, dst = o_stage, a_edge.at[pl.ds(slot * local, local)]

            @pl.when((core == slot) & (q != 3 * f))
            def _():
                act(remote(src, dst, ss.at[0], rs.at[1 + slot], base + 2 * f + y), None)
        @pl.when(q == 3 * f)
        def _():
            act(None, pltpu.make_async_copy(o_stage, a_edge.at[pl.ds(f * local, local)], rs.at[1 + f]))
        for i in range(2):
            src, dst = a_stage.at[pl.ds(i * local, local)], o_edge
            if i == 1 - f:
                here = (y == 1 - f) & (core == 1 - f)
                away = (y == 1 - f) & (core != 1 - f)

                @pl.when(here)
                def _():
                    act(None, pltpu.make_async_copy(src, dst, rs.at[0]))
            else:
                away = y == 1 - f

            @pl.when(away)
            def _():
                act(remote(src, dst, ss.at[1 + i], rs.at[0], base + 2 * core + i), None)

        @pl.when(y == f)
        def _():
            act(remote(a_stage, a_edge, ss.at[3], rs.at[1], base + 2 * (1 - f) + core), None)

    def edges_arrive(f, o_stage, a_stage, o_edge, a_edge, ss, rs):
        to = base + lax.rem(q + 1, 4)
        remote(o_stage, o_edge, ss.at[0], rs.at[0], to).wait_recv()

        @pl.when(y == f)
        def _():
            for slot in range(2):
                remote(o_stage, a_edge.at[pl.ds(slot * local, local)], ss.at[0], rs.at[1 + slot], to).wait_recv()

        @pl.when(y != f)
        def _():
            remote(a_stage, a_edge, ss.at[3], rs.at[1], to).wait_recv()

    e_edges = (1, own.e_stage, moved.e_stage, own.e_edge, moved.e_edge, ees, eer)
    h_edges = (0, own.h_stage, moved.h_stage, own.h_edge, moved.h_edge, hhs, hhr)

    def start(far, near):
        (far or near).start()

    def sent(far, near):
        if far is not None:
            far.wait_send()

    lane = lax.broadcasted_iota(jnp.int32, (BLOCK, width), 1)
    not_end = lane < width - 1
    not_start = lane > 0

    def next_z(f):
        return jnp.where(not_end, pltpu.roll(f, width - 1, 1), 0.0)

    def prev_z(f):
        return jnp.where(not_start, pltpu.roll(f, 1, 1), 0.0)

    shifts = (next_z, prev_z)
    sequence = [c ^ 1 for c in range(CHUNKS)]

    loads[0].wait()
    own.clear(table)
    loads[1].wait()
    for c in sequence:
        own.send_e(c).start()
    wait_in(0)
    for c in sequence:
        moved.send_e(c).start()
    own.stage_e()
    moved.stage_e()
    wait_in(1)
    moved.clear(table)
    edges(*e_edges, start)
    loads[2].wait()
    wait_in(2)

    def store(k, ref, out):
        rows = pl.ds(0, keep)
        skip = pl.ds(PAD if k else 0, keep)
        return pltpu.make_async_copy(ref.at[:, :, :, skip], out.at[:, :, :, rows], out_sem.at[k])

    def each_move_out(k, ref, out, act):
        for half in range(2):
            rows = pl.ds(keep + half * part, part)
            for i in range(2):
                src = ref.at[:, :, pl.ds(i * local, local), pl.ds(PAD if k else 0, part)]
                dst = out.at[:, :, :, rows]
                away = y == half
                if i == half:
                    @pl.when((y == half) & (core == half))
                    def _():
                        act(None, pltpu.make_async_copy(src, dst, ro.at[k, half]))
                    away = away & (core != half)

                @pl.when(away)
                def _():
                    act(remote(src, dst, so.at[k, i], ro.at[k, half], base + 2 * core + i), None)

    def wait_out(k, ref, out):
        for half in range(2):
            src = ref.at[:, :, pl.ds(0, local), pl.ds(PAD if k else 0, part)]
            dst = out.at[:, :, :, pl.ds(keep + half * part, part)]
            remote(src, dst, so.at[k, 0], ro.at[k, half], base + lax.rem(q + 1, 4)).wait_recv()

    @pl.loop(0, ITERS)
    def _(step):
        for c in sequence:
            if c == CHUNKS - 1:
                edges_arrive(*e_edges)
                for tile in tiles:
                    tile.take_e()
            for tile in tiles:
                @pl.when(step > 0)
                def _():
                    tile.send_h(c).wait_send()
                tile.send_e(c).wait_recv()
                tile.sweep(tile.magnetic, range(tile.planes - 1, -1, -1), c, shifts)
                tile.send_h(c).start()
            if c == CHUNKS - 1:
                @pl.when(step > 0)
                def _():
                    edges(*h_edges, sent)
                for tile in tiles:
                    tile.stage_h()
                edges(*h_edges, start)

        @pl.when(step == ITERS - 1)
        def _():
            store(1, own.h, h_out).start()
            each_move_out(1, moved.h, h_out, start)

        for c in sequence:
            if c == 0:
                edges_arrive(*h_edges)
                for tile in tiles:
                    tile.take_h()
            for tile in tiles:
                tile.send_e(c).wait_send()
                tile.send_h(c).wait_recv()
                tile.sweep(tile.electric, range(tile.planes), c, shifts)

                @pl.when(step < ITERS - 1)
                def _():
                    tile.send_e(c).start()
            if c == 0:
                edges(*e_edges, sent)

                @pl.when(step < ITERS - 1)
                def _():
                    for tile in tiles:
                        tile.stage_e()
                    edges(*e_edges, start)

    store(0, own.e, e_out).start()
    each_move_out(0, moved.e, e_out, start)
    each_move_in(sent)
    edges(*h_edges, sent)
    for c in range(CHUNKS):
        for tile in tiles:
            tile.send_h(c).wait_send()
    for k, ref, mref, out in ((0, own.e, moved.e, e_out), (1, own.h, moved.h, h_out)):
        store(k, ref, out).wait()
        each_move_out(k, mref, out, sent)
        wait_out(k, mref, out)


def shards(e_field, h_field, labels, kpoint, eps_inf, delta_eps, omega_zero, damping):
    theta_x = jnp.float32(2.0 * math.pi) * kpoint[0].astype(jnp.float32) / KGRID
    theta_y = jnp.float32(2.0 * math.pi) * kpoint[1].astype(jnp.float32) / KGRID
    cos_x, sin_x = (jnp.cos(theta_x), jnp.sin(theta_x))
    cos_y, sin_y = (jnp.cos(theta_y), jnp.sin(theta_y))
    half = damping * time_step / 2.0
    table = jnp.stack([
        time_step / eps_inf,
        (1.0 - half) / (1.0 + half),
        time_step * omega_zero * omega_zero / (1.0 + half),
        delta_eps,
    ])
    position = lax.axis_index("gx")
    at_first = position == 0
    at_last = position == lax.axis_size("gx") - 1
    one, nought = jnp.float32(1.0), jnp.float32(0.0)
    size = lax.axis_size("gx")
    y = lax.rem(lax.div(position, 2), 2)
    moved_first = (position < 4) & (lax.rem(position, 2) == 0)
    moved_last = (position >= size - 4) & (lax.rem(position, 2) == 1)

    def turn(where, cosv, sinv):
        return [jnp.where(where, cosv, one), jnp.where(where, sinv, nought)]

    phase = jnp.stack(
        turn(at_last, cos_x, sin_x) + turn(at_first, cos_x, -sin_x)
        + turn(moved_last, cos_x, sin_x) + turn(moved_first, cos_x, -sin_x)
        + [cos_y, sin_y] + turn(y == 1, cos_y, sin_y))
    planes, rows, width = labels.shape
    state = (2, 3, planes, rows, width)

    def tile_scratch(planes, rows):
        field = (2, 3, planes, rows, width)
        padded = (2, 3, planes, rows + PAD, width)
        return ([pltpu.VMEM(shape, jnp.float32) for shape in (padded, padded, field, field, (4, planes, rows, width))]
                + [pltpu.VMEM((planes, rows, width), jnp.int32)]
                + [pltpu.VMEM((2, 2, rows, width), jnp.float32)] * 2
                + [pltpu.VMEM((planes, 8, width), jnp.float32)] * 4)

    dma = pltpu.SemaphoreType.DMA
    anywhere = pl.BlockSpec(memory_space=pl.ANY)
    scalars = pl.BlockSpec(memory_space=pltpu.SMEM)
    return pl.pallas_call(
        kernel,
        out_shape=(jax.ShapeDtypeStruct(state, jnp.float32),) * 2,
        in_specs=[anywhere] * 3 + [scalars] * 2,
        out_specs=(anywhere, anywhere),
        scratch_shapes=tile_scratch(planes, rows // 2) + tile_scratch(2 * planes, rows // 4)
        + [dma((CHUNKS,))] * 8
        + [dma((3,)), dma((2,)), dma((3, 2)), dma((3, 2)), dma((2, 2)), dma((2, 2))]
        + [dma((4,)), dma((3,)), dma((4,)), dma((3,))],
        compiler_params=pltpu.CompilerParams(collective_id=0, has_side_effects=True),
    )(e_field, h_field, labels, table, phase)


def solution(mesh):
    placed = (
        P(None, None, ("kpt", "gx"), None, None),
        P(None, None, ("kpt", "gx"), None, None),
        P(("kpt", "gx"), None, None),
        P("kpt"),
        P(),
        P(),
        P(),
        P(),
    )
    return jax.shard_map(
        shards,
        mesh=mesh,
        in_specs=placed,
        out_specs=(
            P(None, None, ("kpt", "gx"), None, None),
            P(None, None, ("kpt", "gx"), None, None),
        ),
        check_vma=False,
    )
```
